32 devices in a mesh: rep: 2 (over x), dp: 16 (over y, z, core).
Axes of the slice: x: 2, y: 2, z: 4, core: 2. Of those that a mesh axis runs over, the one named last changes fastest.
Arguments:
- g_w_gate: bfloat16 [32, 2, 1280, 5120], P(('rep', 'dp')), parts along dimension 0
- g_w_up: bfloat16 [32, 2, 1280, 5120], P(('rep', 'dp')), parts along dimension 0
- g_w_down: bfloat16 [32, 2, 5120, 1280], P(('rep', 'dp')), parts along dimension 0
- w_gate: bfloat16 [2, 1280, 5120], replicated
- w_up: bfloat16 [2, 1280, 5120], replicated
- w_down: bfloat16 [2, 5120, 1280], replicated
- m_w_gate: float32 [2, 1280, 5120], P(None, 'dp')
- m_w_up: float32 [2, 1280, 5120], P(None, 'dp')
- m_w_down: float32 [2, 5120, 1280], P(None, 'dp')
- v_w_gate: float32 [2, 1280, 5120], P(None, 'dp')
- v_w_up: float32 [2, 1280, 5120], P(None, 'dp')
- v_w_down: float32 [2, 5120, 1280], P(None, 'dp')
Outputs:
- output 1: bfloat16 [4, 1280, 5120], P('rep'), parts along dimension 0
- output 2: bfloat16 [4, 1280, 5120], P('rep'), parts along dimension 0
- output 3: bfloat16 [4, 5120, 1280], P('rep'), parts along dimension 0
- output 4: float32 [4, 1280, 5120], P('rep', 'dp'), parts along dimension 0
- output 5: float32 [4, 1280, 5120], P('rep', 'dp'), parts along dimension 0
- output 6: float32 [4, 5120, 1280], P('rep', 'dp'), parts along dimension 0
- output 7: float32 [4, 1280, 5120], P('rep', 'dp'), parts along dimension 0
- output 8: float32 [4, 1280, 5120], P('rep', 'dp'), parts along dimension 0
- output 9: float32 [4, 5120, 1280], P('rep', 'dp'), parts along dimension 0
There are 2 independent parts. The reference program is written for one: setup_inputs(seed, part) draws one part's arguments, and reference() takes and returns one part's arrays. A program takes and returns all parts, laid end to end along the dimension named above; an argument that names none is the same for every part.
All inputs are finite; a program needn't handle non-finite values.
Results may differ from the reference program's by a relative error of at most 0.022.
Values are sent between devices in bfloat16 or wider.
A program may use at most 2 GiB of HBM per device.

```python
import jax
import jax.numpy as jnp
from jax import lax

DEVICES = 16
D = 1280
FF = 5120
LAYERS = 2
NAMES = ("w_gate", "w_up", "w_down")
SHAPES = {"w_gate": (LAYERS, D, FF), "w_up": (LAYERS, D, FF), "w_down": (LAYERS, FF, D)}


def setup_inputs(seed: int = 0, part: int = 0) -> dict:
    kz, *keys = jax.random.split(jax.random.key(seed), 1 + 5 * len(NAMES))
    loud = 2.0 ** jax.random.uniform(kz, (), jnp.float32, -1.0, 1.0)
    drawn = {}
    for name, key, both in zip(NAMES, keys[:3], keys[3:6], strict=True):
        own = jax.random.normal(jax.random.fold_in(key, part), (DEVICES, *SHAPES[name]), jnp.float32)
        shared = jax.random.normal(jax.random.fold_in(both, part), SHAPES[name], jnp.float32)
        drawn["g_" + name] = (loud * (0.7 * shared / DEVICES + 0.7 * own * DEVICES**-0.5)).astype(jnp.bfloat16)
    for name, key in zip(NAMES, keys[6:9], strict=True):
        drawn[name] = (jax.random.normal(key, SHAPES[name], jnp.float32) * SHAPES[name][1] ** -0.5).astype(jnp.bfloat16)
    for name, key in zip(NAMES, keys[9:12], strict=True):
        drawn["m_" + name] = loud * 0.5 * jax.random.normal(key, SHAPES[name], jnp.float32)
    for name, key in zip(NAMES, keys[12:15], strict=True):
        drawn["v_" + name] = loud * loud * jax.random.uniform(key, SHAPES[name], jnp.float32, 0.5, 1.5)
    return drawn


def adamw(w, m, v, g):
    m = 0.9 * m + 0.1 * g
    v = 0.95 * v + 0.05 * g * g
    step = m * lax.rsqrt(v + 1e-8) + 0.1 * w
    return (w - 0.02 * step).astype(jnp.bfloat16), m, v


def clipped(gradients, sum_of_squares, count):
    factor = jnp.minimum(1.0, 0.5 * lax.rsqrt(sum_of_squares / count + 1e-30))
    return [g * factor for g in gradients]


def reference(g_w_gate, g_w_up, g_w_down, w_gate, w_up, w_down, m_w_gate, m_w_up, m_w_down, v_w_gate, v_w_up, v_w_down):
    def total(terms):
        return lax.scan(lambda so_far, term: (so_far + term.astype(jnp.float32), None), jnp.zeros(terms.shape[1:], jnp.float32), terms)[0]

    gradients = [total(terms).astype(jnp.bfloat16).astype(jnp.float32) for terms in (g_w_gate, g_w_up, g_w_down)]
    gradients = clipped(gradients, sum(jnp.sum(g * g) for g in gradients), sum(g.size for g in gradients))
    new = [
        adamw(w.astype(jnp.float32), m, v, g)
        for w, m, v, g in zip((w_gate, w_up, w_down), (m_w_gate, m_w_up, m_w_down), (v_w_gate, v_w_up, v_w_down), gradients, strict=True)
    ]
    return tuple(one[which] for which in range(3) for one in new)
```

```python
import functools

import jax
import jax.numpy as jnp
from jax import lax
from jax.experimental import pallas as pl
from jax.experimental.pallas import tpu as pltpu
from jax.sharding import PartitionSpec as P

MESH = pl.DeviceIdType.MESH
BF16, F32 = jnp.bfloat16, jnp.float32
CHIPS = 8
ROWS = 16
COLS = 1280


def adamw(w, m, v, g):
    m = 0.9 * m + 0.1 * g
    v = 0.95 * v + 0.05 * g * g
    step = m * lax.rsqrt(v + 1e-8) + 0.1 * w
    return (w - 0.02 * step).astype(BF16), m, v


def ring_place(chip):
    return lax.select(chip < 4, chip, 11 - chip)


def each_tile(shape, body):
    rows, cols = shape

    def one(i, _):
        for c in range(cols // COLS):
            body(pl.ds(pl.multiple_of(i * ROWS, ROWS), ROWS), pl.ds(c * COLS, COLS))
        return 0

    lax.fori_loop(0, rows // ROWS, one, 0)


def scatter_kernel(sizes, *refs):
    n = len(sizes)
    terms, refs = refs[:n], refs[n:]
    outs, refs = refs[:n], refs[n:]
    squares, refs = refs[0], refs[1:]
    lent, refs = refs[:n], refs[n:]
    ring, refs = refs[:n], refs[n:]
    own, refs = refs[:n], refs[n:]
    other, refs = refs[:n], refs[n:]
    came, refs = refs[:n], refs[n:]
    held, refs = refs[:n], refs[n:]
    acc, totals, lend_s, lend_r, ring_s, ring_r, load_own, load_other, load_came, norm_s, norm_r = refs

    me = lax.axis_index("dp")
    core, chip = lax.rem(me, 2), lax.div(me, 2)
    place = ring_place(chip)
    way = 1 - 2 * core
    partner = chip * 2 + 1 - core
    following = ring_place(lax.rem(place + way + CHIPS, CHIPS)) * 2 + core
    jobs = [(k, layer) for k in range(n) for layer in range(2)]

    def rows_of(k, block):
        return pl.ds(pl.multiple_of(block * sizes[k][0], 16), sizes[k][0])

    def block_at(step, c):
        at = lax.rem(place - (1 - 2 * c) * (1 + step) + 2 * CHIPS, CHIPS)
        return ring_place(at) * 2 + c

    def lend(step, j):
        k, layer = jobs[j]
        return pltpu.make_async_remote_copy(
            src_ref=terms[k].at[layer, rows_of(k, block_at(step, 1 - core))],
            dst_ref=lent[k].at[step, layer],
            send_sem=lend_s.at[j],
            recv_sem=lend_r.at[step, j],
            device_id={"dp": partner},
            device_id_type=MESH,
        )

    def pass_on(step, j):
        k, layer = jobs[j]
        return pltpu.make_async_remote_copy(
            src_ref=held[k].at[layer],
            dst_ref=ring[k].at[step, layer],
            send_sem=ring_s.at[j],
            recv_sem=ring_r.at[step, j],
            device_id={"dp": following},
            device_id_type=MESH,
        )

    def get_own(step, j):
        k, layer = jobs[j]
        return pltpu.make_async_copy(terms[k].at[layer, rows_of(k, block_at(step, core))], own[k].at[layer], load_own.at[j])

    def get_other(step, j):
        k, layer = jobs[j]
        return pltpu.make_async_copy(lent[k].at[step, layer], other[k].at[layer], load_other.at[j])

    def get_came(step, j):
        k, layer = jobs[j]
        return pltpu.make_async_copy(ring[k].at[step, layer], came[k].at[layer], load_came.at[j])

    barrier = pltpu.get_barrier_semaphore()

    def greet(i, _):
        pl.semaphore_signal(barrier, inc=1, device_id={"dp": lax.rem(me + i, 16)}, device_id_type=MESH)
        return 0

    lax.fori_loop(1, 16, greet, 0)
    for j in range(len(jobs)):
        get_own(0, j).start()
    acc[...] = jnp.zeros_like(acc)
    pl.semaphore_wait(barrier, 15)
    for j in range(len(jobs)):
        lend(0, j).start()

    def one(step, j, first, last):
        k, layer = jobs[j]
        a, b, c, h = (ref[k].at[layer] for ref in (own, other, came, outs if last else held))
        lend(step, j).wait_recv()
        get_other(step, j).start()
        if not first:
            pass_on(step - 1, j).wait_recv()
            get_came(step - 1, j).start()
        lend(step, j).wait_send()
        if not last:
            lend(step + 1, j).start()
        if not first:
            pass_on(step - 1, j).wait_send()
        get_own(step, j).wait()
        get_other(step, j).wait()
        if not first:
            get_came(step - 1, j).wait()

        def add(r, c_):
            so_far = a[r, c_].astype(F32) + b[r, c_].astype(F32)
            if not first:
                so_far = so_far + c[r, c_].astype(F32)
            rounded = so_far.astype(BF16)
            h[r, c_] = rounded
            if last:
                g = rounded.astype(F32)
                acc[...] += g * g

        each_tile(sizes[k], add)
        if not last:
            pass_on(step, j).start()
            get_own(step + 1, j).start()

    for j in range(len(jobs)):
        one(0, j, True, False)

    def middle(step, _):
        for j in range(len(jobs)):
            one(step, j, False, False)
        return 0

    lax.fori_loop(1, CHIPS - 1, middle, 0)
    for j in range(len(jobs)):
        one(CHIPS - 1, j, False, True)

    mine = jnp.zeros((8, 128), F32)
    for r in range(ROWS // 8):
        for c in range(COLS // 128):
            mine = mine + acc[r * 8 : r * 8 + 8, c * 128 : c * 128 + 128]
    totals[me] = mine

    def tell(i):
        return pltpu.make_async_remote_copy(
            src_ref=totals.at[me],
            dst_ref=totals.at[me],
            send_sem=norm_s.at[i],
            recv_sem=norm_r.at[i],
            device_id={"dp": lax.rem(me + i, 16)},
            device_id_type=MESH,
        )

    for i in range(1, 16):
        tell(i).start()
    for i in range(1, 16):
        tell(i).wait()
    total = totals[0]
    for i in range(1, 16):
        total = total + totals[i]
    squares[...] = total


def scatter(terms, sizes):
    n = len(sizes)
    hbm = pl.BlockSpec(memory_space=pltpu.HBM)
    slots = lambda count: [jax.ShapeDtypeStruct((count, 2, *s), BF16) for s in sizes]
    vmem = [pltpu.VMEM((2, *s), BF16) for s in sizes]
    dma = pltpu.SemaphoreType.DMA
    jobs = 2 * n
    out = pl.pallas_call(
        functools.partial(scatter_kernel, sizes),
        out_shape=[
            *(jax.ShapeDtypeStruct((2, *s), BF16) for s in sizes),
            jax.ShapeDtypeStruct((8, 128), F32),
            *slots(CHIPS),
            *slots(CHIPS - 1),
        ],
        in_specs=[hbm] * n,
        out_specs=[pl.BlockSpec(memory_space=pltpu.VMEM)] * (n + 1) + [hbm] * (2 * n),
        scratch_shapes=[
            *vmem * 4,
            pltpu.VMEM((ROWS, COLS), F32),
            pltpu.VMEM((16, 8, 128), F32),
            dma((jobs,)),
            dma((CHIPS, jobs)),
            dma((jobs,)),
            dma((CHIPS - 1, jobs)),
            dma((jobs,)),
            dma((jobs,)),
            dma((jobs,)),
            dma((16,)),
            dma((16,)),
        ],
        compiler_params=pltpu.CompilerParams(collective_id=0, has_side_effects=True, vmem_limit_bytes=40 << 20),
        cost_estimate=pl.CostEstimate(flops=400_000_000, bytes_accessed=300_000_000, transcendentals=0),
        name="scatter_sum",
    )(*terms)
    return out[:n], jnp.sum(out[n])


def copy_kernel(src, dst):
    dst[...] = src[...]


def put_layers(gathered, shape):
    layers, rows, cols = shape
    block = pl.BlockSpec((1, rows // 8, cols), lambda i, j: (i, j, 0))
    return pl.pallas_call(
        copy_kernel,
        grid=(layers, 8),
        out_shape=jax.ShapeDtypeStruct(shape, BF16),
        in_specs=[block],
        out_specs=block,
        compiler_params=pltpu.CompilerParams(vmem_limit_bytes=16 << 20),
        cost_estimate=pl.CostEstimate(flops=40_000_000, bytes_accessed=4 * layers * rows * cols, transcendentals=0),
        name="put_layers",
    )(gathered)


def solution(mesh):
    def step(*arrays):
        terms, weights, m, v = (arrays[i : i + 3] for i in (0, 3, 6, 9))
        sizes = tuple(one.shape[1:] for one in m)
        sums, squares = scatter([t[0] for t in terms], sizes)
        count = 16 * sum(g.size for g in sums)
        factor = jnp.minimum(1.0, 0.5 * lax.rsqrt(squares / count + 1e-30))
        me = lax.axis_index("dp")
        own = [lax.dynamic_slice_in_dim(w, me * one.shape[1], one.shape[1], 1).astype(F32) for w, one in zip(weights, m, strict=True)]
        new = [adamw(w, m, v, g.astype(F32) * factor) for w, m, v, g in zip(own, m, v, sums, strict=True)]
        whole = []
        for one, w in zip(new, weights, strict=True):
            gathered = lax.all_gather(one[0], "dp", axis=1, tiled=True)
            whole.append(put_layers(gathered, w.shape))
        return (*whole, *(one[1] for one in new), *(one[2] for one in new))

    all_of, cut = P(None, None, None), P(None, "dp", None)
    return jax.shard_map(
        step,
        mesh=mesh,
        in_specs=(P(("rep", "dp"), None, None, None),) * 3 + (all_of,) * 3 + (cut,) * 6,
        out_specs=(P("rep", None, None),) * 3 + (P("rep", "dp", None),) * 6,
        check_vma=False,
    )
```

```python
import functools

import jax
import jax.numpy as jnp
from jax import lax
from jax.experimental import pallas as pl
from jax.experimental.pallas import tpu as pltpu
from jax.sharding import PartitionSpec as P

MESH = pl.DeviceIdType.MESH
BF16, F32 = jnp.bfloat16, jnp.float32
CHIPS = 8
HOPS = 5
VMEM_LIMIT = 60 * 1024 * 1024
SLOTS, LAG = 8, 4
ROWS = 16
COLS = 1280


def moments(m, v, g):
    return 0.9 * m + 0.1 * g, 0.95 * v + 0.05 * g * g


def adamw(w, m, v, g):
    m, v = moments(m, v, g)
    step = m * lax.rsqrt(v + 1e-8) + 0.1 * w
    return (w - 0.02 * step).astype(BF16)


def ring_place(chip):
    return lax.select(chip < 4, chip, 11 - chip)


def each_tile(shape, body):
    rows, cols = shape

    def one(i, _):
        for c in range(cols // COLS):
            body(pl.ds(pl.multiple_of(i * ROWS, ROWS), ROWS), pl.ds(c * COLS, COLS))
        return 0

    lax.fori_loop(0, rows // ROWS, one, 0)


def step_kernel(sizes, *refs):
    n = len(sizes)
    refs = list(refs)

    def take(count):
        taken = refs[:count]
        del refs[:count]
        return taken

    terms, weights, old_m, old_v = take(n), take(n), take(n), take(n)
    sums, edges, (factor_ref,), whole, lent, ring = take(n), take(n), take(1), take(n), take(n), take(n)
    own, other, came, held, final, m_in, v_in = (take(n) for _ in range(7))
    acc, totals, lend_s, lend_r, ring_s, ring_r, load_own, load_other, load_came, load_m, load_v, store, norm_s, norm_r = refs

    me = lax.axis_index("dp")
    core, chip = lax.rem(me, 2), lax.div(me, 2)
    place = ring_place(chip)
    way = 1 - 2 * core
    partner = chip * 2 + 1 - core
    following = ring_place(lax.rem(place + way + CHIPS, CHIPS)) * 2 + core
    jobs = [(k, layer) for k in range(n) for layer in range(2)]
    every = range(len(jobs))

    def rows_of(k, block):
        return pl.ds(pl.multiple_of(block * sizes[k][0], 16), sizes[k][0])

    def block_at(step, c):
        at = lax.rem(place - (1 - 2 * c) * (1 + step) + 2 * CHIPS, CHIPS)
        return ring_place(at) * 2 + c

    def remote(src, dst, send, recv, to):
        return pltpu.make_async_remote_copy(
            src_ref=src, dst_ref=dst, send_sem=send, recv_sem=recv, device_id={"dp": to}, device_id_type=MESH
        )

    def lend(step, j):
        k, layer = jobs[j]
        src = terms[k].at[layer, rows_of(k, block_at(step, 1 - core))]
        return remote(src, lent[k].at[step, layer], lend_s.at[j], lend_r.at[step, j], partner)

    def pass_on(step, j):
        k, layer = jobs[j]
        return remote(held[k].at[layer], ring[k].at[step, layer], ring_s.at[j], ring_r.at[step, j], following)

    def get_own(step, j):
        k, layer = jobs[j]
        return pltpu.make_async_copy(terms[k].at[layer, rows_of(k, block_at(step, core))], own[k].at[layer], load_own.at[j])

    def get_other(step, j):
        k, layer = jobs[j]
        return pltpu.make_async_copy(lent[k].at[step, layer], other[k].at[layer], load_other.at[j])

    def get_came(step, j):
        k, layer = jobs[j]
        return pltpu.make_async_copy(ring[k].at[step, layer], came[k].at[layer], load_came.at[j])

    def get_state(j):
        k, layer = jobs[j]
        return (
            pltpu.make_async_copy(old_m[k].at[layer], m_in[k].at[layer], load_m.at[j]),
            pltpu.make_async_copy(old_v[k].at[layer], v_in[k].at[layer], load_v.at[j]),
        )

    def get_weight(j):
        k, layer = jobs[j]
        return pltpu.make_async_copy(weights[k].at[layer, rows_of(k, me)], came[k].at[layer], load_came.at[j])

    def put_sum(j):
        k, layer = jobs[j]
        return pltpu.make_async_copy(final[k].at[layer], sums[k].at[layer], load_own.at[j])

    barrier = pltpu.get_barrier_semaphore()

    def greet(i, _):
        pl.semaphore_signal(barrier, inc=1, device_id={"dp": lax.rem(me + i, 16)}, device_id_type=MESH)
        return 0

    lax.fori_loop(1, 16, greet, 0)
    for j in every:
        get_own(0, j).start()
    acc[...] = jnp.zeros_like(acc)
    pl.semaphore_wait(barrier, 15)
    for j in every:
        lend(0, j).start()

    def one(step, j, first, last):
        k, layer = jobs[j]
        a, b, c, h = (ref[k].at[layer] for ref in (own, other, came, final if last else held))
        lend(step, j).wait_recv()
        get_other(step, j).start()
        if not first:
            pass_on(step - 1, j).wait_recv()
            get_came(step - 1, j).start()
        lend(step, j).wait_send()
        if not last:
            lend(step + 1, j).start()
        if not first:
            pass_on(step - 1, j).wait_send()
        get_own(step, j).wait()
        get_other(step, j).wait()
        if not first:
            get_came(step - 1, j).wait()

        def add(r, c_):
            so_far = a[r, c_].astype(F32) + b[r, c_].astype(F32)
            if not first:
                so_far = so_far + c[r, c_].astype(F32)
            rounded = so_far.astype(BF16)
            h[r, c_] = rounded
            if last:
                g = rounded.astype(F32)
                acc[...] += g * g

        each_tile(sizes[k], add)
        if not last:
            pass_on(step, j).start()
            get_own(step + 1, j).start()
        else:
            get_weight(j).start()
            put_sum(j).start()

    for j in every:
        one(0, j, True, False)
    for j in every:
        for copy in get_state(j):
            copy.start()

    def middle(step, _):
        for j in every:
            one(step, j, False, False)
        return 0

    lax.fori_loop(1, CHIPS - 1, middle, 0)
    for j in every:
        one(CHIPS - 1, j, False, True)

    mine = jnp.zeros((8, 128), F32)
    for r in range(ROWS // 8):
        for c in range(COLS // 128):
            mine = mine + acc[r * 8 : r * 8 + 8, c * 128 : c * 128 + 128]
    totals[me] = mine

    def tell(i):
        return remote(totals.at[me], totals.at[me], norm_s.at[i], norm_r.at[i], lax.rem(me + i, 16))

    for i in range(1, 16):
        tell(i).start()
    for j in every:
        get_weight(j).wait()
        for copy in get_state(j):
            copy.wait()
    for i in range(1, 16):
        tell(i).wait()
    total = totals[0]
    for i in range(1, 16):
        total = total + totals[i]
    count = 16 * 2 * sum(rows * cols for rows, cols in sizes)
    factor_ref[...] = jnp.minimum(1.0, 0.5 * lax.rsqrt(jnp.full((8, 128), jnp.sum(total)) / count + 1e-30))
    factor = jnp.max(factor_ref[...])

    def rows_at(k, h):
        return rows_of(k, ring_place(lax.rem(place - way * h + CHIPS, CHIPS)) * 2 + core)

    def block_of(h, j):
        k, layer = jobs[j]
        first = isinstance(h, int) and h == 0
        return held[k].at[layer] if first else whole[k].at[layer, rows_at(k, h)]

    def hop(h, j, to_edge=False):
        k, layer = jobs[j]
        dst = edges[k].at[layer] if to_edge else whole[k].at[layer, rows_at(k, h)]
        return remote(block_of(h, j), dst, ring_s.at[j], ring_r.at[h, j], following)

    def give(h, j):
        k, layer = jobs[j]
        return remote(block_of(h, j), whole[k].at[layer, rows_at(k, h)], lend_s.at[j], lend_r.at[h, j], partner)

    def keep(j):
        k, layer = jobs[j]
        return pltpu.make_async_copy(block_of(0, j), whole[k].at[layer, rows_at(k, 0)], store.at[j])

    for j in every:
        k, layer = jobs[j]
        a, w, m, v, h = (ref[k].at[layer] for ref in (final, came, m_in, v_in, held))

        def update(r, c_):
            h[r, c_] = adamw(w[r, c_].astype(F32), m[r, c_], v[r, c_], a[r, c_].astype(F32) * factor)

        each_tile(sizes[k], update)
        hop(0, j).start()
        give(0, j).start()
        keep(j).start()

    def along(h, _):
        for j in every:
            hop(h - 1, j).wait()
            hop(h, j).start()
            give(h - 1, j).wait()
            give(h, j).start()
        return 0

    lax.fori_loop(1, HOPS - 1, along, 0)
    last = HOPS - 1
    for j in every:
        hop(last - 1, j).wait()
        hop(last, j, True).start()
        give(last - 1, j).wait()
        give(last, j).start()
    for j in every:
        keep(j).wait()
        put_sum(j).wait()
        give(last, j).wait()
    for j in every:
        hop(last, j, True).wait()


def step_call(terms, weights, m, v):
    n = len(terms)
    sizes = tuple(one.shape[1:] for one in m)
    hbm, vmem = pl.BlockSpec(memory_space=pltpu.HBM), pl.BlockSpec(memory_space=pltpu.VMEM)
    arrays = lambda count: [jax.ShapeDtypeStruct((*count, 2, *s), BF16) for s in sizes]
    buffers = lambda kind: [pltpu.VMEM((2, *s), kind) for s in sizes]
    dma = pltpu.SemaphoreType.DMA
    jobs = 2 * n
    out = pl.pallas_call(
        functools.partial(step_kernel, sizes),
        out_shape=[
            *arrays(()),
            *arrays(()),
            jax.ShapeDtypeStruct((8, 128), F32),
            *(jax.ShapeDtypeStruct(w.shape, BF16) for w in weights),
            *arrays((CHIPS,)),
            *arrays((CHIPS - 1,)),
        ],
        in_specs=[hbm] * (4 * n),
        out_specs=[hbm] * (2 * n) + [vmem] + [hbm] * (3 * n),
        scratch_shapes=[
            *buffers(BF16) * 5,
            *buffers(F32) * 2,
            pltpu.VMEM((ROWS, COLS), F32),
            pltpu.VMEM((16, 8, 128), F32),
            dma((jobs,)),
            dma((CHIPS, jobs)),
            dma((jobs,)),
            dma((CHIPS - 1, jobs)),
            *[dma((jobs,))] * 6,
            dma((16,)),
            dma((16,)),
        ],
        compiler_params=pltpu.CompilerParams(collective_id=0, has_side_effects=True, vmem_limit_bytes=VMEM_LIMIT),
        cost_estimate=pl.CostEstimate(flops=400_000_000, bytes_accessed=300_000_000, transcendentals=0),
        name="step_kernel",
    )(*terms, *weights, *m, *v)
    return out[:n], out[n : 2 * n], out[2 * n][0, 0], out[2 * n + 1 : 3 * n + 1]


def move(tasks, slots, load, store):
    def read(t):
        return pltpu.make_async_copy(tasks[t][0], slots.at[t % SLOTS], load.at[t % SLOTS])

    def write(t):
        return pltpu.make_async_copy(slots.at[t % SLOTS], tasks[t][1], store.at[t % SLOTS])

    count = len(tasks)
    for t in range(count + LAG):
        if t < count:
            if t >= SLOTS:
                write(t - SLOTS).wait()
            read(t).start()
        if t >= LAG:
            read(t - LAG).wait()
            write(t - LAG).start()
    for t in range(max(0, count - SLOTS), count):
        write(t).wait()


def rows_back(h, rows, mine):
    me = lax.axis_index("dp")
    core, place = lax.rem(me, 2), ring_place(lax.div(me, 2))
    of = core if mine else 1 - core
    block = ring_place(lax.rem(place - (1 - 2 * of) * h + CHIPS, CHIPS)) * 2 + of
    return pl.ds(pl.multiple_of(block * rows, 16), rows)


def fill_kernel(rows, whole, edge, edge_given, came, given, out, slots, load, store):
    tasks = []
    for layer in range(2):
        for mine in (True, False):
            for h in range(HOPS):
                at = out.at[layer, rows_back(h, rows, mine)]
                tasks.append((whole.at[layer, rows_back(h, rows, mine)], at))
        for h, mine, src in ((HOPS, True, edge), (HOPS, False, edge_given), (HOPS + 1, True, came), (HOPS + 1, False, given)):
            tasks.append((src.at[layer], out.at[layer, rows_back(h, rows, mine)]))
    move(tasks, slots, load, store)


def finish_kernel(rows, _, came, given, out, slots, load, store):
    tasks = []
    for layer in range(2):
        for mine, src in ((True, came), (False, given)):
            tasks.append((src.at[layer], out.at[layer, rows_back(HOPS + 2, rows, mine)]))
    move(tasks, slots, load, store)


def local_call(kernel, arrays, block, aliases, flops):
    hbm = pl.BlockSpec(memory_space=pltpu.HBM)
    return pl.pallas_call(
        functools.partial(kernel, block[0]),
        out_shape=jax.ShapeDtypeStruct(arrays[0].shape, BF16),
        in_specs=[hbm] * len(arrays),
        out_specs=hbm,
        input_output_aliases=aliases,
        scratch_shapes=[
            pltpu.VMEM((SLOTS, *block), BF16),
            pltpu.SemaphoreType.DMA((SLOTS,)),
            pltpu.SemaphoreType.DMA((SLOTS,)),
        ],
        compiler_params=pltpu.CompilerParams(vmem_limit_bytes=VMEM_LIMIT),
        cost_estimate=pl.CostEstimate(flops=flops, bytes_accessed=arrays[0].size * 4, transcendentals=0),
    )(*arrays)


def permute(arrays, pairs):
    out = []
    for one in arrays:
        out.append(lax.ppermute(one, "dp", pairs))
    return out


def solution(mesh):
    place = lambda chip: chip if chip < 4 else 11 - chip
    onward = [(2 * q + c, 2 * place((place(q) + 1 - 2 * c) % CHIPS) + c) for q in range(CHIPS) for c in range(2)]
    across = [(i, i ^ 1) for i in range(2 * CHIPS)]

    def step(*arrays):
        terms, weights, m, v = (arrays[i : i + 3] for i in (0, 3, 6, 9))
        sums, edges, factor, gathered = step_call([t[0] for t in terms], weights, m, v)
        came = permute(edges, onward)
        last = permute(came, onward)
        edge_given, given = permute(edges, across), permute(came, across)
        last_given = permute(last, across)
        new = [moments(a, b, g.astype(F32) * factor) for a, b, g in zip(m, v, sums, strict=True)]
        whole = []
        for k, one in enumerate(m):
            block = one.shape[1:]
            w = local_call(fill_kernel, (gathered[k], edges[k], edge_given[k], came[k], given[k]), block, {}, 60_000_000)
            whole.append(local_call(finish_kernel, (w, last[k], last_given[k]), block, {0: 0}, 8_000_000))
        return (*whole, *(one[0] for one in new), *(one[1] for one in new))

    all_of, cut = P(None, None, None), P(None, "dp", None)
    return jax.shard_map(
        step,
        mesh=mesh,
        in_specs=(P(("rep", "dp"), None, None, None),) * 3 + (all_of,) * 3 + (cut,) * 6,
        out_specs=(P("rep", None, None),) * 3 + (P("rep", "dp", None),) * 6,
        check_vma=False,
    )
```

```python
import functools

import jax
import jax.numpy as jnp
from jax import lax
from jax.experimental import pallas as pl
from jax.experimental.pallas import tpu as pltpu
from jax.sharding import PartitionSpec as P

MESH = pl.DeviceIdType.MESH
BF16, F32 = jnp.bfloat16, jnp.float32
CHIPS = 8
HOPS = 5
VMEM_LIMIT = 60 * 1024 * 1024
SLOTS, LAG = 8, 4
ROWS = 16
COLS = 1280


def moments(m, v, g):
    return 0.9 * m + 0.1 * g, 0.95 * v + 0.05 * g * g


def adamw(w, m, v, g):
    m, v = moments(m, v, g)
    step = m * lax.rsqrt(v + 1e-8) + 0.1 * w
    return (w - 0.02 * step).astype(BF16)


def ring_place(chip):
    return lax.select(chip < 4, chip, 11 - chip)


STREAMS = ((0, (0, 1)), (1, (0, 1)), (2, (0,)), (2, (1,)))


def each_tile(shape, body, first=0, count=None):
    rows, cols = shape
    count = rows // ROWS if count is None else count

    def one(i, _):
        for c in range(cols // COLS):
            body(pl.ds(pl.multiple_of(i * ROWS, ROWS), ROWS), pl.ds(c * COLS, COLS))
        return 0

    lax.fori_loop(first, first + count, one, 0)


def step_kernel(sizes, *refs):
    n = len(sizes)
    refs = list(refs)

    def take(count):
        taken = refs[:count]
        del refs[:count]
        return taken

    terms, weights, old_m, old_v = take(n), take(n), take(n), take(n)
    sums, edges, (factor_ref,), whole, lent, ring = take(n), take(len(STREAMS)), take(1), take(n), take(n), take(n)
    own, other, came, held, final, late, m_in, v_in = (take(n) for _ in range(8))
    acc, totals, lend_s, lend_r, ring_s, ring_r, load_own, load_other, load_came, load_m, load_v, store, norm_s, norm_r, first_r = refs

    me = lax.axis_index("dp")
    core, chip = lax.rem(me, 2), lax.div(me, 2)
    place = ring_place(chip)
    way = 1 - 2 * core
    partner = chip * 2 + 1 - core
    following = ring_place(lax.rem(place + way + CHIPS, CHIPS)) * 2 + core
    jobs = [(k, layer) for k in range(n) for layer in range(2)]
    every = range(len(jobs))
    edge_of = {(k, layer): edges[e].at[i] for e, (k, layers) in enumerate(STREAMS) for i, layer in enumerate(layers)}
    pieces = [pl.ds(i * ROWS, ROWS) for i in range(sizes[0][0] // ROWS)]

    def rows_of(k, block):
        return pl.ds(pl.multiple_of(block * sizes[k][0], 16), sizes[k][0])

    def block_at(step, c):
        at = lax.rem(place - (1 - 2 * c) * (1 + step) + 2 * CHIPS, CHIPS)
        return ring_place(at) * 2 + c

    def remote(src, dst, send, recv, to):
        return pltpu.make_async_remote_copy(
            src_ref=src, dst_ref=dst, send_sem=send, recv_sem=recv, device_id={"dp": to}, device_id_type=MESH
        )

    def lend(step, j):
        k, layer = jobs[j]
        src = terms[k].at[layer, rows_of(k, block_at(step, 1 - core))]
        dst = other[k].at[layer] if isinstance(step, int) and step == 0 else lent[k].at[step - 1, layer]
        return remote(src, dst, lend_s.at[j], lend_r.at[step, j], partner)

    def lend_piece(i):
        return remote(came[0].at[0, pieces[i]], other[0].at[0, pieces[i]], lend_s.at[0], first_r.at[i], partner)

    def pass_on(step, j):
        k, layer = jobs[j]
        dst = late[k].at[layer] if isinstance(step, int) and step == CHIPS - 2 else ring[k].at[step, layer]
        return remote(held[k].at[layer], dst, ring_s.at[j], ring_r.at[step, j], following)

    def pass_piece(i):
        return remote(held[0].at[0, pieces[i]], ring[0].at[0, 0, pieces[i]], ring_s.at[0], ring_r.at[0, 0], following)

    def get_own(step, j):
        k, layer = jobs[j]
        return pltpu.make_async_copy(terms[k].at[layer, rows_of(k, block_at(step, core))], own[k].at[layer], load_own.at[j])

    def get_other(step, j):
        k, layer = jobs[j]
        return pltpu.make_async_copy(lent[k].at[step - 1, layer], other[k].at[layer], load_other.at[j])

    def get_came(step, j):
        k, layer = jobs[j]
        return pltpu.make_async_copy(ring[k].at[step, layer], came[k].at[layer], load_came.at[j])

    def get_state(j):
        k, layer = jobs[j]
        return (
            pltpu.make_async_copy(old_m[k].at[layer], m_in[k].at[layer], load_m.at[j]),
            pltpu.make_async_copy(old_v[k].at[layer], v_in[k].at[layer], load_v.at[j]),
        )

    def get_weight(j):
        k, layer = jobs[j]
        return pltpu.make_async_copy(weights[k].at[layer, rows_of(k, me)], came[k].at[layer], load_came.at[j])

    def put_sum(j):
        k, layer = jobs[j]
        return pltpu.make_async_copy(final[k].at[layer], sums[k].at[layer], load_own.at[j])

    barrier = pltpu.get_barrier_semaphore()

    def greet(i, _):
        pl.semaphore_signal(barrier, inc=1, device_id={"dp": lax.rem(me + i, 16)}, device_id_type=MESH)
        return 0

    lax.fori_loop(1, 16, greet, 0)
    first_lent = pltpu.make_async_copy(terms[0].at[0, rows_of(0, block_at(0, 1 - core))], came[0].at[0], load_came.at[0])
    first_lent.start()
    for j in every:
        get_own(0, j).start()
    acc[...] = jnp.zeros_like(acc)
    first_lent.wait()
    pl.semaphore_wait(barrier, 15)
    for i in range(len(pieces)):
        lend_piece(i).start()
    for j in every[1:]:
        lend(0, j).start()

    def one(step, j, first, last):
        k, layer = jobs[j]
        a, b = own[k].at[layer], other[k].at[layer]
        c, h = (late if last else came)[k].at[layer], (final if last else held)[k].at[layer]
        cut = first and j == 0
        if not cut:
            lend(step, j).wait_recv()
        if not first:
            get_other(step, j).start()
            pass_on(step - 1, j).wait_recv()
            if not last:
                get_came(step - 1, j).start()
        if not cut:
            lend(step, j).wait_send()
            if not last:
                lend(step + 1, j).start()
        if not first:
            pass_on(step - 1, j).wait_send()
        get_own(step, j).wait()
        if not first:
            get_other(step, j).wait()
            if not last:
                get_came(step - 1, j).wait()

        def add(r, c_):
            so_far = a[r, c_].astype(F32) + b[r, c_].astype(F32)
            if not first:
                so_far = so_far + c[r, c_].astype(F32)
            rounded = so_far.astype(BF16)
            h[r, c_] = rounded
            if last:
                g = rounded.astype(F32)
                acc[...] += g * g

        if cut:
            for i in range(len(pieces)):
                lend_piece(i).wait_recv()
                each_tile(sizes[k], add, i, 1)
                pass_piece(i).start()
            lend(step, j).wait_send()
            lend(step + 1, j).start()
        else:
            each_tile(sizes[k], add)
        if not last:
            if not cut:
                pass_on(step, j).start()
            get_own(step + 1, j).start()
        else:
            get_weight(j).start()
            put_sum(j).start()

    for j in every:
        one(0, j, True, False)
    for j in every:
        for copy in get_state(j):
            copy.start()

    def middle(step, _):
        for j in every:
            one(step, j, False, False)
        return 0

    lax.fori_loop(1, CHIPS - 2, middle, 0)
    for j in every:
        one(CHIPS - 2, j, False, False)
    for j in every:
        one(CHIPS - 1, j, False, True)

    mine = jnp.zeros((8, 128), F32)
    for r in range(ROWS // 8):
        for c in range(COLS // 128):
            mine = mine + acc[r * 8 : r * 8 + 8, c * 128 : c * 128 + 128]
    totals[me] = mine

    def tell(i):
        return remote(totals.at[me], totals.at[me], norm_s.at[i], norm_r.at[i], lax.rem(me + i, 16))

    for i in range(1, 16):
        tell(i).start()
    for j in every:
        get_weight(j).wait()
        for copy in get_state(j):
            copy.wait()
    for i in range(1, 16):
        tell(i).wait()
    total = totals[0]
    for i in range(1, 16):
        total = total + totals[i]
    count = 16 * 2 * sum(rows * cols for rows, cols in sizes)
    factor_ref[...] = jnp.minimum(1.0, 0.5 * lax.rsqrt(jnp.full((8, 128), jnp.sum(total)) / count + 1e-30))
    factor = jnp.max(factor_ref[...])

    def rows_at(k, h):
        return rows_of(k, ring_place(lax.rem(place - way * h + CHIPS, CHIPS)) * 2 + core)

    def block_of(h, j):
        k, layer = jobs[j]
        first = isinstance(h, int) and h == 0
        return held[k].at[layer] if first else whole[k].at[layer, rows_at(k, h)]

    def hop(h, j, to_edge=False):
        k, layer = jobs[j]
        dst = edge_of[jobs[j]] if to_edge else whole[k].at[layer, rows_at(k, h)]
        return remote(block_of(h, j), dst, ring_s.at[j], ring_r.at[h, j], following)

    def hop_piece(i):
        block = rows_at(0, 0)
        dst = whole[0].at[0, pl.ds(pl.multiple_of(block.start + i * ROWS, ROWS), ROWS)]
        return remote(held[0].at[0, pieces[i]], dst, ring_s.at[0], ring_r.at[0, 0], following)

    def give(h, j):
        k, layer = jobs[j]
        return remote(block_of(h, j), whole[k].at[layer, rows_at(k, h)], lend_s.at[j], lend_r.at[h, j], partner)

    def keep(j):
        k, layer = jobs[j]
        return pltpu.make_async_copy(block_of(0, j), whole[k].at[layer, rows_at(k, 0)], store.at[j])

    for j in every:
        k, layer = jobs[j]
        a, w, m, v, h = (ref[k].at[layer] for ref in (final, came, m_in, v_in, held))

        def update(r, c_):
            h[r, c_] = adamw(w[r, c_].astype(F32), m[r, c_], v[r, c_], a[r, c_].astype(F32) * factor)

        if j == 0:
            for i in range(len(pieces)):
                each_tile(sizes[k], update, i, 1)
                hop_piece(i).start()
        else:
            each_tile(sizes[k], update)
            hop(0, j).start()
        give(0, j).start()
        keep(j).start()

    def along(h, _):
        for j in every:
            hop(h - 1, j).wait()
            hop(h, j).start()
            give(h - 1, j).wait()
            give(h, j).start()
        return 0

    lax.fori_loop(1, HOPS - 1, along, 0)
    last = HOPS - 1
    for j in every:
        hop(last - 1, j).wait()
        hop(last, j, True).start()
        give(last - 1, j).wait()
        give(last, j).start()
    for j in every:
        keep(j).wait()
        put_sum(j).wait()
        give(last, j).wait()
    for j in every:
        hop(last, j, True).wait()


def step_call(terms, weights, m, v):
    n = len(terms)
    sizes = tuple(one.shape[1:] for one in m)
    hbm, vmem = pl.BlockSpec(memory_space=pltpu.HBM), pl.BlockSpec(memory_space=pltpu.VMEM)
    arrays = lambda count: [jax.ShapeDtypeStruct((*count, 2, *s), BF16) for s in sizes]
    buffers = lambda kind: [pltpu.VMEM((2, *s), kind) for s in sizes]
    dma = pltpu.SemaphoreType.DMA
    jobs = 2 * n
    out = pl.pallas_call(
        functools.partial(step_kernel, sizes),
        out_shape=[
            *arrays(()),
            *(jax.ShapeDtypeStruct((len(layers), *sizes[k]), BF16) for k, layers in STREAMS),
            jax.ShapeDtypeStruct((8, 128), F32),
            *(jax.ShapeDtypeStruct(w.shape, BF16) for w in weights),
            *arrays((CHIPS - 1,)),
            *arrays((CHIPS - 2,)),
        ],
        in_specs=[hbm] * (4 * n),
        out_specs=[hbm] * (n + len(STREAMS)) + [vmem] + [hbm] * (3 * n),
        scratch_shapes=[
            *buffers(BF16) * 6,
            *buffers(F32) * 2,
            pltpu.VMEM((ROWS, COLS), F32),
            pltpu.VMEM((16, 8, 128), F32),
            dma((jobs,)),
            dma((CHIPS, jobs)),
            dma((jobs,)),
            dma((CHIPS - 1, jobs)),
            *[dma((jobs,))] * 6,
            dma((16,)),
            dma((16,)),
            dma((sizes[0][0] // ROWS,)),
        ],
        compiler_params=pltpu.CompilerParams(collective_id=0, has_side_effects=True, vmem_limit_bytes=VMEM_LIMIT),
        cost_estimate=pl.CostEstimate(flops=400_000_000, bytes_accessed=300_000_000, transcendentals=0),
        name="step_kernel",
    )(*terms, *weights, *m, *v)
    cut = n + len(STREAMS)
    return out[:n], out[n:cut], out[cut][0, 0], out[cut + 1 : cut + 1 + n]


def move(tasks, slots, load, store):
    def read(t):
        return pltpu.make_async_copy(tasks[t][0], slots.at[t % SLOTS], load.at[t % SLOTS])

    def write(t):
        return pltpu.make_async_copy(slots.at[t % SLOTS], tasks[t][1], store.at[t % SLOTS])

    count = len(tasks)
    for t in range(count + LAG):
        if t < count:
            if t >= SLOTS:
                write(t - SLOTS).wait()
            read(t).start()
        if t >= LAG:
            read(t - LAG).wait()
            write(t - LAG).start()
    for t in range(max(0, count - SLOTS), count):
        write(t).wait()


def rows_back(h, rows, mine):
    me = lax.axis_index("dp")
    core, place = lax.rem(me, 2), ring_place(lax.div(me, 2))
    of = core if mine else 1 - core
    block = ring_place(lax.rem(place - (1 - 2 * of) * h + CHIPS, CHIPS)) * 2 + of
    return pl.ds(pl.multiple_of(block * rows, 16), rows)


def fill_kernel(k, rows, whole, *refs):
    *streams, out, slots, load, store = refs
    tasks = []
    for layer in range(2):
        for mine in (True, False):
            for h in range(HOPS):
                at = rows_back(h, rows, mine)
                tasks.append((whole.at[layer, at], out.at[layer, at]))
    for i, layers in enumerate(layers for of, layers in STREAMS if of == k):
        for h, mine, src in zip((HOPS, HOPS, HOPS + 1, HOPS + 1), (True, False) * 2, streams[4 * i : 4 * i + 4], strict=True):
            for at, layer in enumerate(layers):
                tasks.append((src.at[at], out.at[layer, rows_back(h, rows, mine)]))
    move(tasks, slots, load, store)


def fill(k, rows, whole, streams):
    hbm = pl.BlockSpec(memory_space=pltpu.HBM)
    return pl.pallas_call(
        functools.partial(fill_kernel, k, rows),
        out_shape=jax.ShapeDtypeStruct(whole.shape, BF16),
        in_specs=[hbm] * (1 + len(streams)),
        out_specs=hbm,
        scratch_shapes=[
            pltpu.VMEM((SLOTS, rows, whole.shape[2]), BF16),
            pltpu.SemaphoreType.DMA((SLOTS,)),
            pltpu.SemaphoreType.DMA((SLOTS,)),
        ],
        compiler_params=pltpu.CompilerParams(vmem_limit_bytes=VMEM_LIMIT),
        cost_estimate=pl.CostEstimate(flops=60_000_000, bytes_accessed=whole.size * 4, transcendentals=0),
        name="fill",
    )(whole, *streams)


def finish_kernel(layers, rows, _, came, given, out, store):
    copies = []
    for at, layer in enumerate(layers):
        for mine, src in ((True, came), (False, given)):
            dst = out.at[layer, rows_back(HOPS + 2, rows, mine)]
            copies.append(pltpu.make_async_copy(src.at[at], dst, store.at[len(copies)]))
    for copy in copies:
        copy.start()
    for copy in copies:
        copy.wait()


def finish(layers, rows, w, came, given):
    hbm, vmem = pl.BlockSpec(memory_space=pltpu.HBM), pl.BlockSpec(memory_space=pltpu.VMEM)
    return pl.pallas_call(
        functools.partial(finish_kernel, layers, rows),
        out_shape=jax.ShapeDtypeStruct(w.shape, BF16),
        in_specs=[hbm, vmem, vmem],
        out_specs=hbm,
        input_output_aliases={0: 0},
        scratch_shapes=[pltpu.SemaphoreType.DMA((2 * len(layers),))],
        compiler_params=pltpu.CompilerParams(vmem_limit_bytes=8 << 20),
        cost_estimate=pl.CostEstimate(flops=8_000_000, bytes_accessed=came.size * 8, transcendentals=0),
        name="finish",
    )(w, came, given)


def permute(arrays, pairs):
    out = []
    for one in arrays:
        out.append(lax.ppermute(one, "dp", pairs))
    return out


def solution(mesh):
    place = lambda chip: chip if chip < 4 else 11 - chip
    onward = [(2 * q + c, 2 * place((place(q) + 1 - 2 * c) % CHIPS) + c) for q in range(CHIPS) for c in range(2)]
    across = [(i, i ^ 1) for i in range(2 * CHIPS)]

    def step(*arrays):
        terms, weights, m, v = (arrays[i : i + 3] for i in (0, 3, 6, 9))
        sums, edges, factor, gathered = step_call([t[0] for t in terms], weights, m, v)
        came = permute(edges, onward)
        last = permute(came, onward)
        edge_given, given = permute(edges, across), permute(came, across)
        last_given = permute(last, across)
        new = [moments(a, b, g.astype(F32) * factor) for a, b, g in zip(m, v, sums, strict=True)]
        whole = list(gathered)
        for k, one in enumerate(m):
            mine = [e for e, (of, _) in enumerate(STREAMS) if of == k]
            streams = [part[e] for e in mine for part in (edges, edge_given, came, given)]
            whole[k] = fill(k, one.shape[1], whole[k], streams)
        for e, (k, layers) in enumerate(STREAMS):
            whole[k] = finish(layers, m[k].shape[1], whole[k], last[e], last_given[e])
        return (*whole, *(one[0] for one in new), *(one[1] for one in new))

    all_of, cut = P(None, None, None), P(None, "dp", None)
    return jax.shard_map(
        step,
        mesh=mesh,
        in_specs=(P(("rep", "dp"), None, None, None),) * 3 + (all_of,) * 3 + (cut,) * 6,
        out_specs=(P("rep", None, None),) * 3 + (P("rep", "dp", None),) * 6,
        check_vma=False,
    )
```

```python
import functools

import jax
import jax.numpy as jnp
from jax import lax
from jax.experimental import pallas as pl
from jax.experimental.pallas import tpu as pltpu
from jax.sharding import PartitionSpec as P

MESH = pl.DeviceIdType.MESH
BF16, F32 = jnp.bfloat16, jnp.float32
CHIPS = 8
HOPS = 5
VMEM_LIMIT = 60 * 1024 * 1024
ENDS = 4
SLOTS, LAG = 8, 4
ROWS = 16
COLS = 1280


def moments(m, v, g):
    return 0.9 * m + 0.1 * g, 0.95 * v + 0.05 * g * g


def adamw(w, m, v, g):
    m, v = moments(m, v, g)
    step = m * lax.rsqrt(v + 1e-8) + 0.1 * w
    return (w - 0.02 * step).astype(BF16)


def ring_place(chip):
    return lax.select(chip < 4, chip, 11 - chip)


STREAMS = ((0, (0, 1)), (1, (0, 1)), (2, (0,)), (2, (1,)))


def each_tile(shape, body, first=0, count=None):
    rows, cols = shape
    count = rows // ROWS if count is None else count

    def one(i, _):
        for c in range(cols // COLS):
            body(pl.ds(pl.multiple_of(i * ROWS, ROWS), ROWS), pl.ds(c * COLS, COLS))
        return 0

    lax.fori_loop(first, first + count, one, 0)


def step_kernel(sizes, *refs):
    n = len(sizes)
    refs = list(refs)

    def take(count):
        taken = refs[:count]
        del refs[:count]
        return taken

    terms, weights, old_m, old_v = take(n), take(n), take(n), take(n)
    sums, edges, (factor_ref,), whole, lent, ring = take(n), take(len(STREAMS)), take(1), take(n), take(n), take(n)
    own, other, came, held, final, late, m_in, v_in = (take(n) for _ in range(8))
    acc, totals, lend_s, lend_r, ring_s, ring_r, load_own, load_other, load_came, load_m, load_v, store, norm_s, norm_r, first_r, late_r = refs

    me = lax.axis_index("dp")
    core, chip = lax.rem(me, 2), lax.div(me, 2)
    place = ring_place(chip)
    way = 1 - 2 * core
    partner = chip * 2 + 1 - core
    following = ring_place(lax.rem(place + way + CHIPS, CHIPS)) * 2 + core
    jobs = [(k, layer) for k in range(n) for layer in range(2)]
    every = range(len(jobs))
    edge_of = {(k, layer): edges[e].at[i] for e, (k, layers) in enumerate(STREAMS) for i, layer in enumerate(layers)}
    pieces = [pl.ds(i * ROWS, ROWS) for i in range(sizes[0][0] // ROWS)]
    end = len(jobs) - 1
    quarter = sizes[-1][0] // ENDS

    def rows_of(k, block):
        return pl.ds(pl.multiple_of(block * sizes[k][0], 16), sizes[k][0])

    def block_at(step, c):
        at = lax.rem(place - (1 - 2 * c) * (1 + step) + 2 * CHIPS, CHIPS)
        return ring_place(at) * 2 + c

    def remote(src, dst, send, recv, to):
        return pltpu.make_async_remote_copy(
            src_ref=src, dst_ref=dst, send_sem=send, recv_sem=recv, device_id={"dp": to}, device_id_type=MESH
        )

    def lend(step, j):
        k, layer = jobs[j]
        src = terms[k].at[layer, rows_of(k, block_at(step, 1 - core))]
        dst = other[k].at[layer] if isinstance(step, int) and step == 0 else lent[k].at[step - 1, layer]
        return remote(src, dst, lend_s.at[j], lend_r.at[step, j], partner)

    def lend_piece(i):
        return remote(came[0].at[0, pieces[i]], other[0].at[0, pieces[i]], lend_s.at[0], first_r.at[i], partner)

    def pass_on(step, j):
        k, layer = jobs[j]
        dst = late[k].at[layer] if isinstance(step, int) and step == CHIPS - 2 else ring[k].at[step, layer]
        return remote(held[k].at[layer], dst, ring_s.at[j], ring_r.at[step, j], following)

    def pass_piece(i):
        return remote(held[0].at[0, pieces[i]], ring[0].at[0, 0, pieces[i]], ring_s.at[0], ring_r.at[0, 0], following)

    def end_piece(i):
        rows = pl.ds(i * quarter, quarter)
        return remote(held[-1].at[1, rows], late[-1].at[1, rows], ring_s.at[end], late_r.at[i], following)

    def get_own(step, j):
        k, layer = jobs[j]
        return pltpu.make_async_copy(terms[k].at[layer, rows_of(k, block_at(step, core))], own[k].at[layer], load_own.at[j])

    def get_other(step, j):
        k, layer = jobs[j]
        return pltpu.make_async_copy(lent[k].at[step - 1, layer], other[k].at[layer], load_other.at[j])

    def get_came(step, j):
        k, layer = jobs[j]
        return pltpu.make_async_copy(ring[k].at[step, layer], came[k].at[layer], load_came.at[j])

    def get_state(j):
        k, layer = jobs[j]
        return (
            pltpu.make_async_copy(old_m[k].at[layer], m_in[k].at[layer], load_m.at[j]),
            pltpu.make_async_copy(old_v[k].at[layer], v_in[k].at[layer], load_v.at[j]),
        )

    def get_weight(j):
        k, layer = jobs[j]
        return pltpu.make_async_copy(weights[k].at[layer, rows_of(k, me)], came[k].at[layer], load_came.at[j])

    def put_sum(j):
        k, layer = jobs[j]
        return pltpu.make_async_copy(final[k].at[layer], sums[k].at[layer], load_own.at[j])

    barrier = pltpu.get_barrier_semaphore()

    def greet(i, _):
        pl.semaphore_signal(barrier, inc=1, device_id={"dp": lax.rem(me + i, 16)}, device_id_type=MESH)
        return 0

    lax.fori_loop(1, 16, greet, 0)
    first_lent = pltpu.make_async_copy(terms[0].at[0, rows_of(0, block_at(0, 1 - core))], came[0].at[0], load_came.at[0])
    first_lent.start()
    for j in every:
        get_own(0, j).start()
    acc[...] = jnp.zeros_like(acc)
    first_lent.wait()
    pl.semaphore_wait(barrier, 15)
    for i in range(len(pieces)):
        lend_piece(i).start()
    for j in every[1:]:
        lend(0, j).start()

    def one(step, j, first, last):
        k, layer = jobs[j]
        a, b = own[k].at[layer], other[k].at[layer]
        c, h = (late if last else came)[k].at[layer], (final if last else held)[k].at[layer]
        cut = first and j == 0
        ending = j == end and isinstance(step, int) and step >= CHIPS - 2
        if not cut:
            lend(step, j).wait_recv()
        if not first:
            get_other(step, j).start()
            if not (last and j == end):
                pass_on(step - 1, j).wait_recv()
            if not last:
                get_came(step - 1, j).start()
        if not cut:
            lend(step, j).wait_send()
            if not last:
                lend(step + 1, j).start()
        if not first:
            pass_on(step - 1, j).wait_send()
        get_own(step, j).wait()
        if not first:
            get_other(step, j).wait()
            if not last:
                get_came(step - 1, j).wait()

        def add(r, c_):
            so_far = a[r, c_].astype(F32) + b[r, c_].astype(F32)
            if not first:
                so_far = so_far + c[r, c_].astype(F32)
            rounded = so_far.astype(BF16)
            h[r, c_] = rounded
            if last:
                g = rounded.astype(F32)
                acc[...] += g * g

        if cut:
            for i in range(len(pieces)):
                lend_piece(i).wait_recv()
                each_tile(sizes[k], add, i, 1)
                pass_piece(i).start()
            lend(step, j).wait_send()
            lend(step + 1, j).start()
        elif ending:
            for i in range(ENDS):
                if last:
                    end_piece(i).wait_recv()
                each_tile(sizes[k], add, i * quarter // ROWS, quarter // ROWS)
                if not last:
                    end_piece(i).start()
        else:
            each_tile(sizes[k], add)
        if not last:
            if not cut and not ending:
                pass_on(step, j).start()
            get_own(step + 1, j).start()
        else:
            get_weight(j).start()
            put_sum(j).start()

    for j in every:
        one(0, j, True, False)
    for j in every:
        for copy in get_state(j):
            copy.start()

    def middle(step, _):
        for j in every:
            one(step, j, False, False)
        return 0

    lax.fori_loop(1, CHIPS - 2, middle, 0)
    for j in every:
        one(CHIPS - 2, j, False, False)
    for j in every:
        one(CHIPS - 1, j, False, True)

    mine = jnp.zeros((8, 128), F32)
    for r in range(ROWS // 8):
        for c in range(COLS // 128):
            mine = mine + acc[r * 8 : r * 8 + 8, c * 128 : c * 128 + 128]
    totals[me] = jnp.broadcast_to(jnp.sum(mine, axis=0, keepdims=True), (8, 128))
    told = totals.at[me, pl.ds(0, 1)]

    def tell(i):
        return remote(told, told, norm_s.at[i], norm_r.at[i], lax.rem(me + i, 16))

    for i in range(1, 16):
        tell(i).start()
    for j in every:
        get_weight(j).wait()
        for copy in get_state(j):
            copy.wait()
    for i in range(1, 16):
        tell(i).wait()
    total = totals[0, 0:1]
    for i in range(1, 16):
        total = total + totals[i, 0:1]
    count = 16 * 2 * sum(rows * cols for rows, cols in sizes)
    factor_ref[...] = jnp.minimum(1.0, 0.5 * lax.rsqrt(jnp.full((8, 128), jnp.sum(total)) / count + 1e-30))
    factor = jnp.max(factor_ref[...])

    def rows_at(k, h):
        return rows_of(k, ring_place(lax.rem(place - way * h + CHIPS, CHIPS)) * 2 + core)

    def block_of(h, j):
        k, layer = jobs[j]
        first = isinstance(h, int) and h == 0
        return held[k].at[layer] if first else whole[k].at[layer, rows_at(k, h)]

    def hop(h, j, to_edge=False):
        k, layer = jobs[j]
        dst = edge_of[jobs[j]] if to_edge else whole[k].at[layer, rows_at(k, h)]
        return remote(block_of(h, j), dst, ring_s.at[j], ring_r.at[h, j], following)

    def hop_piece(i):
        block = rows_at(0, 0)
        dst = whole[0].at[0, pl.ds(pl.multiple_of(block.start + i * ROWS, ROWS), ROWS)]
        return remote(held[0].at[0, pieces[i]], dst, ring_s.at[0], ring_r.at[0, 0], following)

    def give(h, j):
        k, layer = jobs[j]
        return remote(block_of(h, j), whole[k].at[layer, rows_at(k, h)], lend_s.at[j], lend_r.at[h, j], partner)

    def keep(j):
        k, layer = jobs[j]
        return pltpu.make_async_copy(block_of(0, j), whole[k].at[layer, rows_at(k, 0)], store.at[j])

    for j in every:
        k, layer = jobs[j]
        a, w, m, v, h = (ref[k].at[layer] for ref in (final, came, m_in, v_in, held))

        def update(r, c_):
            h[r, c_] = adamw(w[r, c_].astype(F32), m[r, c_], v[r, c_], a[r, c_].astype(F32) * factor)

        if j == 0:
            for i in range(len(pieces)):
                each_tile(sizes[k], update, i, 1)
                hop_piece(i).start()
        else:
            each_tile(sizes[k], update)
            hop(0, j).start()
        give(0, j).start()
        keep(j).start()

    def along(h, _):
        for j in every:
            hop(h - 1, j).wait()
            hop(h, j).start()
            give(h - 1, j).wait()
            give(h, j).start()
        return 0

    lax.fori_loop(1, HOPS - 1, along, 0)
    last = HOPS - 1
    for j in every:
        hop(last - 1, j).wait()
        hop(last, j, True).start()
        give(last - 1, j).wait()
        give(last, j).start()
    for j in every:
        keep(j).wait()
        put_sum(j).wait()
        give(last, j).wait()
    for j in every:
        hop(last, j, True).wait()


def step_call(terms, weights, m, v):
    n = len(terms)
    sizes = tuple(one.shape[1:] for one in m)
    hbm, vmem = pl.BlockSpec(memory_space=pltpu.HBM), pl.BlockSpec(memory_space=pltpu.VMEM)
    arrays = lambda count: [jax.ShapeDtypeStruct((*count, 2, *s), BF16) for s in sizes]
    buffers = lambda kind: [pltpu.VMEM((2, *s), kind) for s in sizes]
    dma = pltpu.SemaphoreType.DMA
    jobs = 2 * n
    out = pl.pallas_call(
        functools.partial(step_kernel, sizes),
        out_shape=[
            *arrays(()),
            *(jax.ShapeDtypeStruct((len(layers), *sizes[k]), BF16) for k, layers in STREAMS),
            jax.ShapeDtypeStruct((8, 128), F32),
            *(jax.ShapeDtypeStruct(w.shape, BF16) for w in weights),
            *arrays((CHIPS - 1,)),
            *arrays((CHIPS - 2,)),
        ],
        in_specs=[hbm] * (4 * n),
        out_specs=[hbm] * (n + len(STREAMS)) + [vmem] + [hbm] * (3 * n),
        scratch_shapes=[
            *buffers(BF16) * 6,
            *buffers(F32) * 2,
            pltpu.VMEM((ROWS, COLS), F32),
            pltpu.VMEM((16, 8, 128), F32),
            dma((jobs,)),
            dma((CHIPS, jobs)),
            dma((jobs,)),
            dma((CHIPS - 1, jobs)),
            *[dma((jobs,))] * 6,
            dma((16,)),
            dma((16,)),
            dma((sizes[0][0] // ROWS,)),
            dma((ENDS,)),
        ],
        compiler_params=pltpu.CompilerParams(collective_id=0, has_side_effects=True, vmem_limit_bytes=VMEM_LIMIT),
        cost_estimate=pl.CostEstimate(flops=400_000_000, bytes_accessed=300_000_000, transcendentals=0),
        name="step_kernel",
    )(*terms, *weights, *m, *v)
    cut = n + len(STREAMS)
    return out[:n], out[n:cut], out[cut][0, 0], out[cut + 1 : cut + 1 + n]


def move(tasks, slots, load, store):
    def read(t):
        return pltpu.make_async_copy(tasks[t][0], slots.at[t % SLOTS], load.at[t % SLOTS])

    def write(t):
        return pltpu.make_async_copy(slots.at[t % SLOTS], tasks[t][1], store.at[t % SLOTS])

    count = len(tasks)
    for t in range(count + LAG):
        if t < count:
            if t >= SLOTS:
                write(t - SLOTS).wait()
            read(t).start()
        if t >= LAG:
            read(t - LAG).wait()
            write(t - LAG).start()
    for t in range(max(0, count - SLOTS), count):
        write(t).wait()


def rows_back(h, rows, mine):
    me = lax.axis_index("dp")
    core, place = lax.rem(me, 2), ring_place(lax.div(me, 2))
    of = core if mine else 1 - core
    block = ring_place(lax.rem(place - (1 - 2 * of) * h + CHIPS, CHIPS)) * 2 + of
    return pl.ds(pl.multiple_of(block * rows, 16), rows)


def fill_kernel(k, rows, whole, *refs):
    *streams, out, slots, load, store = refs
    tasks = []
    for layer in range(2):
        for mine in (True, False):
            for h in range(HOPS):
                at = rows_back(h, rows, mine)
                tasks.append((whole.at[layer, at], out.at[layer, at]))
    for i, layers in enumerate(layers for of, layers in STREAMS if of == k):
        for h, mine, src in zip((HOPS, HOPS, HOPS + 1, HOPS + 1), (True, False) * 2, streams[4 * i : 4 * i + 4], strict=True):
            for at, layer in enumerate(layers):
                tasks.append((src.at[at], out.at[layer, rows_back(h, rows, mine)]))
    move(tasks, slots, load, store)


def fill(k, rows, whole, streams):
    hbm = pl.BlockSpec(memory_space=pltpu.HBM)
    return pl.pallas_call(
        functools.partial(fill_kernel, k, rows),
        out_shape=jax.ShapeDtypeStruct(whole.shape, BF16),
        in_specs=[hbm] * (1 + len(streams)),
        out_specs=hbm,
        scratch_shapes=[
            pltpu.VMEM((SLOTS, rows, whole.shape[2]), BF16),
            pltpu.SemaphoreType.DMA((SLOTS,)),
            pltpu.SemaphoreType.DMA((SLOTS,)),
        ],
        compiler_params=pltpu.CompilerParams(vmem_limit_bytes=VMEM_LIMIT),
        cost_estimate=pl.CostEstimate(flops=60_000_000, bytes_accessed=whole.size * 4, transcendentals=0),
        name="fill",
    )(whole, *streams)


def finish_kernel(layers, rows, whose, _, *refs):
    *parts, out, store = refs
    copies = []
    for at, layer in enumerate(layers):
        for mine, src in zip(whose, parts, strict=True):
            dst = out.at[layer, rows_back(HOPS + 2, rows, mine)]
            copies.append(pltpu.make_async_copy(src.at[at], dst, store.at[len(copies)]))
    for copy in copies:
        copy.start()
    for copy in copies:
        copy.wait()


def finish(layers, rows, w, whose, parts):
    hbm, vmem = pl.BlockSpec(memory_space=pltpu.HBM), pl.BlockSpec(memory_space=pltpu.VMEM)
    return pl.pallas_call(
        functools.partial(finish_kernel, layers, rows, whose),
        out_shape=jax.ShapeDtypeStruct(w.shape, BF16),
        in_specs=[hbm] + [vmem] * len(parts),
        out_specs=hbm,
        input_output_aliases={0: 0},
        scratch_shapes=[pltpu.SemaphoreType.DMA((len(parts) * len(layers),))],
        compiler_params=pltpu.CompilerParams(vmem_limit_bytes=8 << 20),
        cost_estimate=pl.CostEstimate(flops=8_000_000, bytes_accessed=parts[0].size * 8, transcendentals=0),
        name="finish",
    )(w, *parts)


def permute(arrays, pairs):
    out = []
    for one in arrays:
        out.append(lax.ppermute(one, "dp", pairs))
    return out


def solution(mesh):
    place = lambda chip: chip if chip < 4 else 11 - chip
    onward = [(2 * q + c, 2 * place((place(q) + 1 - 2 * c) % CHIPS) + c) for q in range(CHIPS) for c in range(2)]
    across = [(i, i ^ 1) for i in range(2 * CHIPS)]

    def step(*arrays):
        terms, weights, m, v = (arrays[i : i + 3] for i in (0, 3, 6, 9))
        sums, edges, factor, gathered = step_call([t[0] for t in terms], weights, m, v)
        came = permute(edges, onward)
        last = permute(came, onward)
        edge_given, given = permute(edges, across), permute(came, across)
        last_given = permute(last, across)
        new = [moments(a, b, g.astype(F32) * factor) for a, b, g in zip(m, v, sums, strict=True)]
        whole = list(gathered)
        for k, one in enumerate(m):
            mine = [e for e, (of, _) in enumerate(STREAMS) if of == k]
            streams = [part[e] for e in mine for part in (edges, edge_given, came, given)]
            whole[k] = fill(k, one.shape[1], whole[k], streams)
        for e, (k, layers) in enumerate(STREAMS):
            both = [(True, last[e]), (False, last_given[e])]
            groups = [[one] for one in both] if e == len(STREAMS) - 1 else [both]
            for group in groups:
                whole[k] = finish(layers, m[k].shape[1], whole[k], *(tuple(x) for x in zip(*group, strict=True)))
        return (*whole, *(one[0] for one in new), *(one[1] for one in new))

    all_of, cut = P(None, None, None), P(None, "dp", None)
    return jax.shard_map(
        step,
        mesh=mesh,
        in_specs=(P(("rep", "dp"), None, None, None),) * 3 + (all_of,) * 3 + (cut,) * 6,
        out_specs=(P("rep", None, None),) * 3 + (P("rep", "dp", None),) * 6,
        check_vma=False,
    )
```
